32 devices in a mesh: gx: 2 (over x), gy: 4 (over y, core), gz: 4 (over z).
Axes of the slice: x: 2, y: 2, z: 4, core: 2. Of those that a mesh axis runs over, the one named last changes fastest.
Arguments:
- features: bfloat16 [256, 4096], P('gz', ('gy', 'gx')), may hold values from -14 to 14, as said below
- tiles: bfloat16 [32, 32, 128, 128], P('gx', 'gy'), may hold values from -0.5 to 0.5
- block_mask: int32 [32, 32], P('gx', 'gy'), may hold values from 0 to 1, as said below
- tile_counts: int32 [32], P('gx'), may hold values from 1 to 32, as said below
- weight: bfloat16 [256, 256], replicated, may hold values from -0.375 to 0.375
- gamma: float32 [256], P('gz'), may hold values from 0.5 to 2
- beta: float32 [256], P('gz'), may hold values from -3 to 3
Outputs:
- normed: bfloat16 [256, 4096], P('gz', ('gx', 'gy'))
The draws below stay inside these ranges and needn't reach their ends.
Inputs may be any that keep to these rules, and one draw needn't show every extreme that they name: `features`: channels along dimension 0, nodes along dimension 1. `block_mask`: 1 where block row and block column meet in a nonzero block, else 0; the diagonal is 1. tile_counts[r] is the number of ones in row r of block_mask.
All inputs are finite; a program needn't handle non-finite values.
Results may differ from the reference program's by a relative error of at most 0.013.
Values may be sent and summed in bfloat16 or wider, within the bound.
A program may use at most 64 MiB of HBM per device.

```python
import math
import jax
import jax.numpy as jnp
from jax import lax

F = 256
TILE = 128
NBLK = 32
NODES = 4096


def shared_mask(key):
    levels = jax.random.randint(jax.random.fold_in(key, 11), (NBLK,), 3, 7)
    limits = jnp.left_shift(jnp.int32(1), levels.astype(jnp.int32))
    draws = jax.random.randint(jax.random.fold_in(key, 12), (NBLK, NBLK), 0, 128)
    mask = (draws < limits[:, None]).astype(jnp.int32)
    eye = jnp.eye(NBLK, dtype=jnp.int32)
    mask = jnp.maximum(mask, eye)
    sparse_row = jax.random.randint(jax.random.fold_in(key, 13), (), 0, NBLK)
    step_ahead = jax.random.randint(jax.random.fold_in(key, 14), (), 1, max(NBLK, 2))
    dense_row = (sparse_row + step_ahead) % NBLK
    row_ids = jnp.arange(NBLK, dtype=jnp.int32)[:, None]
    mask = jnp.where(row_ids == dense_row, jnp.ones_like(mask), mask)
    mask = jnp.where(row_ids == sparse_row, eye, mask)
    return mask


def draw_block_mask(key, part):
    return shared_mask(key)


def draw_tile_counts(key, part):
    return jnp.sum(shared_mask(key), axis=1).astype(jnp.int32)


def draw_features(key, part):
    position = jnp.arange(NODES, dtype=jnp.float32)
    rising = 1.0 + 2.0 * position / max(NODES - 1, 1)
    values = jnp.clip(jax.random.normal(key, (F, NODES), jnp.float32), -4.5, 4.5)
    return (values * rising[None, :]).astype(jnp.bfloat16)


def shard_levels(stream_key, shape, split, smallest, top_value):
    def one(axis_at, shards_of):
        heights = jax.random.uniform(jax.random.fold_in(jax.random.fold_in(stream_key, 6), axis_at), (shards_of,), jnp.float32, smallest / len(split), top_value / len(split))
        return jnp.repeat(jnp.exp(heights), shape[axis_at] // shards_of).reshape((-1,) + (1,) * (len(shape) - axis_at - 1))

    factor_of = one(*split[0])
    for cut in split[1:]:
        factor_of = factor_of * one(*cut)
    return factor_of


def noise(key, shape, deviation, limit, cuts=(), kind=jnp.bfloat16):
    gain = shard_levels(key, shape, cuts, -0.22, 0.18) if cuts else 1.0
    drawn = jax.random.normal(key, shape, jnp.float32) * deviation * gain
    return jnp.minimum(jnp.maximum(drawn, -limit), limit).astype(kind)


def setup_inputs(seed: int = 0) -> dict:
    keys = jax.random.split(jax.random.key(seed), 8)
    return {
        "features": draw_features(jax.random.fold_in(keys[7], 71), 0),
        "tiles": noise(keys[1], (NBLK, NBLK, TILE, TILE), TILE ** -0.5, 0.5, ((0, 2), (1, 4))),
        "block_mask": draw_block_mask(jax.random.fold_in(keys[7], 71), 0),
        "tile_counts": draw_tile_counts(jax.random.fold_in(keys[7], 71), 0),
        "weight": noise(keys[4], (F, F), F ** -0.5, 0.375),
        "gamma": jnp.clip(jnp.exp(math.log(2.0) - 1.3862944 * jax.random.uniform(keys[5], (F,), jnp.float32) ** shard_levels(keys[5], (F,), ((0, 4),), -0.2, 0.2)), 0.5, 2.0),
        "beta": noise(keys[6], (F,), 0.5, 3.0, ((0, 4),), jnp.float32),
    }


def reference(features, tiles, block_mask, tile_counts, weight, gamma, beta):
    panels = features.astype(jnp.float32).reshape(F, NBLK, TILE)

    def one_row(index):
        block = lax.dynamic_index_in_dim(tiles, index, 0, keepdims=False).astype(jnp.float32)
        prods = jnp.einsum('fcn,cmn->fcm', panels, block)
        mask_row = lax.dynamic_index_in_dim(block_mask, index, 0, keepdims=False).astype(jnp.float32)
        count = lax.dynamic_index_in_dim(tile_counts, index, 0, keepdims=False).astype(jnp.float32)
        share = mask_row / count
        return jnp.einsum('fcm,c->fm', prods, share)
    rows_out = lax.map(one_row, jnp.arange(NBLK, dtype=jnp.int32))
    agg = jnp.transpose(rows_out, (1, 0, 2)).reshape(F, NODES).astype(jnp.bfloat16)
    z_vals = jnp.dot(weight.T, agg, preferred_element_type=jnp.float32)
    mean = lax.optimization_barrier(jnp.sum(z_vals, axis=1)) / NODES
    centered = z_vals - mean[:, None]
    var = lax.optimization_barrier(jnp.sum(centered * centered, axis=1)) / NODES
    scaled = gamma[:, None] * centered * lax.rsqrt(var + 1e-05)[:, None] + beta[:, None]
    return jnp.maximum(scaled, 0.0).astype(jnp.bfloat16)
```

```python
import functools

import jax
import jax.numpy as jnp
from jax import lax
from jax.experimental import pallas as pl
from jax.experimental.pallas import tpu as pltpu
from jax.sharding import PartitionSpec as P

MESH = pl.DeviceIdType.MESH
CHUNKS = 2


def kernel(
    sizes, chunks,
    feat_hbm, tiles_hbm, mask_ref, count_ref, weight_hbm, gamma_hbm, beta_hbm,
    out_ref,
    panel, tiles, weight, w_rows, gamma, beta, acc, mine, part_out, part_in, full, z_scr,
    stat_out, stat_in,
    load_sem, tile_sem, x_send, x_recv, y_send, y_recv, z_send, z_recv, s_send, s_recv,
):
    nx, ny, nz = sizes
    gx, gy, gz = lax.axis_index("gx"), lax.axis_index("gy"), lax.axis_index("gz")
    rows_blk, cols_blk, tile_len, _ = tiles.shape
    local_ch = panel.shape[1]
    cpl = cols_blk // nx
    rpd = rows_blk // ny
    rc = rpd // chunks
    span = rc * tile_len
    f32, bf16 = jnp.float32, jnp.bfloat16

    loads = [
        pltpu.make_async_copy(feat_hbm, panel.at[gx], load_sem.at[0]),
        pltpu.make_async_copy(weight_hbm, weight, load_sem.at[1]),
        pltpu.make_async_copy(gamma_hbm, gamma, load_sem.at[2]),
        pltpu.make_async_copy(beta_hbm, beta, load_sem.at[3]),
    ]
    loads[0].start()
    tile_loads = {}
    for s in range(nx):
        col = lax.rem(gx + s, nx) * cpl
        for g in range(ny):
            tile_loads[s, g] = pltpu.make_async_copy(
                tiles_hbm.at[pl.ds(g * rpd, rpd), pl.ds(col, cpl)],
                tiles.at[pl.ds(g * rpd, rpd), pl.ds(col, cpl)],
                tile_sem.at[s, g],
            )

    barrier = pltpu.get_barrier_semaphore()
    xy_peers = [
        (lax.rem(gx + i, nx), lax.rem(gy + j, ny), gz)
        for i in range(nx) for j in range(ny) if i or j
    ]
    z_peers = [(gx, gy, lax.rem(gz + k, nz)) for k in range(1, nz)]
    for peer in xy_peers + z_peers:
        pl.semaphore_signal(barrier, inc=1, device_id=peer, device_id_type=MESH)
    for g in range(ny):
        tile_loads[0, g].start()
    for load in loads[1:]:
        load.start()
    for s in range(1, nx):
        for g in range(ny):
            tile_loads[s, g].start()
    loads[0].wait()
    pl.semaphore_wait(barrier, len(xy_peers) + len(z_peers))

    x_copies = []
    for s in range(1, nx):
        copy = pltpu.make_async_remote_copy(
            src_ref=panel.at[gx], dst_ref=panel.at[gx],
            send_sem=x_send.at[s - 1], recv_sem=x_recv.at[s - 1],
            device_id=(lax.rem(gx + s, nx), gy, gz), device_id_type=MESH,
        )
        copy.start()
        x_copies.append(copy)

    loads[1].wait()
    w_rows[...] = weight[...].T
    for load in loads[2:]:
        load.wait()

    def product(r, src):
        lhs, rhs = [], []
        for j in range(cpl):
            flag = mask_ref[r, src * cpl + j].astype(f32)
            block = panel[src, :, j * tile_len:(j + 1) * tile_len]
            lhs.append(block * jnp.full(block.shape, flag, f32).astype(bf16))
            rhs.append(tiles[r, src * cpl + j])
        return lax.dot_general(
            jnp.concatenate(lhs, axis=1), jnp.concatenate(rhs, axis=1),
            (((1,), (1,)), ((), ())), preferred_element_type=f32,
        )

    for g in range(ny):
        tile_loads[0, g].wait()
        for i in range(rpd):
            acc[g * rpd + i] = product(g * rpd + i, gx)
    for s in range(1, nx):
        for g in range(ny):
            tile_loads[s, g].wait()
        src = lax.rem(gx + nx - s, nx)
        x_copies[s - 1].wait()
        if s < nx - 1:
            for r in range(rows_blk):
                acc[r] += product(r, src)
    last = lax.rem(gx + 1, nx)

    y_copies = {}
    for h in range(chunks):
        for k in list(range(1, ny)) + [0]:
            dest = lax.rem(gy + k, ny)
            for i in range(rc):
                r = dest * rpd + h * rc + i
                total = acc[r]
                if nx > 1:
                    total = total + product(r, last)
                count = jnp.full(total.shape, count_ref[r].astype(f32), f32)
                total = total / count
                cols = slice(i * tile_len, (i + 1) * tile_len)
                if k:
                    part_out[k - 1, h, :, cols] = total.astype(bf16)
                else:
                    mine[h, :, cols] = total
            if k:
                copy = pltpu.make_async_remote_copy(
                    src_ref=part_out.at[k - 1, h], dst_ref=part_in.at[k - 1, h],
                    send_sem=y_send.at[k - 1, h], recv_sem=y_recv.at[k - 1, h],
                    device_id=(gx, dest, gz), device_id_type=MESH,
                )
                copy.start()
                y_copies[k, h] = copy

    z_copies = {}
    ch = pl.ds(pl.multiple_of(gz * local_ch, local_ch), local_ch)
    for h in range(chunks):
        total = mine[h]
        for k in range(1, ny):
            y_copies[k, h].wait_recv()
            total = total + part_in[k - 1, h].astype(f32)
        full[h, ch, :] = total.astype(bf16)
        for k in range(1, nz):
            copy = pltpu.make_async_remote_copy(
                src_ref=full.at[h, ch], dst_ref=full.at[h, ch],
                send_sem=z_send.at[k - 1, h], recv_sem=z_recv.at[k - 1, h],
                device_id=z_peers[k - 1], device_id_type=MESH,
            )
            copy.start()
            z_copies[k, h] = copy

    w_local = w_rows[ch, :]
    sums = jnp.zeros((local_ch, 1), f32)
    squares = jnp.zeros((local_ch, 1), f32)
    for h in range(chunks):
        for k in range(1, nz):
            z_copies[k, h].wait_recv()
        z_vals = jnp.dot(w_local, full[h], preferred_element_type=f32)
        z_scr[h] = z_vals
        sums += jnp.sum(z_vals, axis=1, keepdims=True)
        squares += jnp.sum(z_vals * z_vals, axis=1, keepdims=True)
    lane = lax.broadcasted_iota(jnp.int32, (local_ch, 128), 1)
    stacked = jnp.where(lane == 0, sums, jnp.where(lane == 1, squares, 0.0))
    stat_out[...] = stacked.T[0:8, :]
    s_copies = []
    for k, peer in enumerate(xy_peers):
        copy = pltpu.make_async_remote_copy(
            src_ref=stat_out, dst_ref=stat_in.at[k],
            send_sem=s_send.at[k], recv_sem=s_recv.at[k],
            device_id=peer, device_id_type=MESH,
        )
        copy.start()
        s_copies.append(copy)
    stats = stat_out[...]
    for k, copy in enumerate(s_copies):
        copy.wait_recv()
        stats = stats + stat_in[k]
    nodes = span * chunks * nx * ny
    mean = stats[0:1, :] / nodes
    var = stats[1:2, :] / nodes - mean * mean
    scale = gamma[...] * lax.rsqrt(var + 1e-05)
    row = lax.broadcasted_iota(jnp.int32, (8, local_ch), 0)
    table = jnp.where(row == 0, mean, jnp.where(row == 1, scale, beta[...]))
    cols = table.T
    mean_c, scale_c, beta_c = cols[:, 0:1], cols[:, 1:2], cols[:, 2:3]
    for h in range(chunks):
        value = (z_scr[h] - mean_c) * scale_c + beta_c
        out_ref[:, h * span:(h + 1) * span] = jnp.maximum(value, 0.0).astype(bf16)

    for copy in list(y_copies.values()) + list(z_copies.values()) + s_copies:
        copy.wait_send()


def body(sizes, features, tiles, block_mask, tile_counts, weight, gamma, beta):
    nx, ny, nz = sizes
    local_ch, nodes = features.shape
    rows_blk, cols_blk, tile_len, _ = tiles.shape
    width = rows_blk * tile_len // ny
    rpd = rows_blk // ny
    chunks = CHUNKS if rpd % CHUNKS == 0 else 1
    span = width // chunks
    f32, bf16 = jnp.float32, jnp.bfloat16
    peers = nx * ny - 1
    dma = pltpu.SemaphoreType.DMA
    hbm = pl.BlockSpec(memory_space=pl.ANY)
    smem = pl.BlockSpec(memory_space=pltpu.SMEM)
    return pl.pallas_call(
        functools.partial(kernel, sizes, chunks),
        out_shape=jax.ShapeDtypeStruct((local_ch, width), bf16),
        in_specs=[hbm, hbm, smem, smem, hbm, hbm, hbm],
        out_specs=pl.BlockSpec(memory_space=pltpu.VMEM),
        scratch_shapes=[
            pltpu.VMEM((nx, local_ch, nodes), bf16),
            pltpu.VMEM(tiles.shape, bf16),
            pltpu.VMEM(weight.shape, bf16),
            pltpu.VMEM(weight.shape[::-1], bf16),
            pltpu.VMEM((1, local_ch), f32),
            pltpu.VMEM((1, local_ch), f32),
            pltpu.VMEM((rows_blk, local_ch, tile_len), f32),
            pltpu.VMEM((chunks, local_ch, span), f32),
            pltpu.VMEM((max(ny - 1, 1), chunks, local_ch, span), bf16),
            pltpu.VMEM((max(ny - 1, 1), chunks, local_ch, span), bf16),
            pltpu.VMEM((chunks, local_ch * nz, span), bf16),
            pltpu.VMEM((chunks, local_ch, span), f32),
            pltpu.VMEM((8, local_ch), f32),
            pltpu.VMEM((max(peers, 1), 8, local_ch), f32),
            dma((4,)),
            dma((nx, ny)),
            dma((max(nx - 1, 1),)),
            dma((max(nx - 1, 1),)),
            dma((max(ny - 1, 1), chunks)),
            dma((max(ny - 1, 1), chunks)),
            dma((max(nz - 1, 1), chunks)),
            dma((max(nz - 1, 1), chunks)),
            dma((max(peers, 1),)),
            dma((max(peers, 1),)),
        ],
        compiler_params=pltpu.CompilerParams(collective_id=0, has_side_effects=True),
        name="graph_conv",
    )(features, tiles, block_mask, tile_counts, weight,
      gamma.reshape(1, local_ch), beta.reshape(1, local_ch))


def solution(mesh):
    in_specs = (
        P("gz", ("gy", "gx")),
        P("gx", "gy", None, None),
        P("gx", "gy"),
        P("gx"),
        P(),
        P("gz"),
        P("gz"),
    )
    out_specs = P("gz", ("gx", "gy"))
    sizes = tuple(mesh.shape[name] for name in ("gx", "gy", "gz"))
    return jax.shard_map(
        functools.partial(body, sizes), mesh=mesh, in_specs=in_specs,
        out_specs=out_specs, check_vma=False,
    )
```

```python
import functools

import jax
import jax.numpy as jnp
from jax import lax
from jax.experimental import pallas as pl
from jax.experimental.pallas import tpu as pltpu
from jax.sharding import PartitionSpec as P

MESH = pl.DeviceIdType.MESH
CHUNKS = 2


def kernel(
    sizes, chunks,
    feat_hbm, tiles_hbm, mask_hbm, count_hbm, weight_hbm, gamma_hbm, beta_hbm,
    out_ref,
    mask_ref, count_ref, panel, tiles, weight, w_rows, gamma, beta, acc, mine, part_out, part_in, full, z_scr,
    stat_out, stat_in,
    load_sem, tile_sem, up_sem, down_sem, x_send, x_recv, y_send, y_recv, z_send, z_recv, s_send, s_recv,
):
    nx, ny, nz = sizes
    gx, gy, gz = lax.axis_index("gx"), lax.axis_index("gy"), lax.axis_index("gz")
    rows_blk, cols_blk, tile_len, _ = tiles.shape
    local_ch = panel.shape[1]
    cpl = cols_blk // nx
    rpd = rows_blk // ny
    rc = rpd // chunks
    span = rc * tile_len
    f32, bf16 = jnp.float32, jnp.bfloat16

    loads = [
        pltpu.make_async_copy(feat_hbm, panel.at[gx], load_sem.at[0]),
        pltpu.make_async_copy(weight_hbm, weight, load_sem.at[1]),
        pltpu.make_async_copy(gamma_hbm, gamma, load_sem.at[2]),
        pltpu.make_async_copy(beta_hbm, beta, load_sem.at[3]),
        pltpu.make_async_copy(mask_hbm, mask_ref, load_sem.at[4]),
        pltpu.make_async_copy(count_hbm, count_ref, load_sem.at[5]),
    ]
    tile_loads = {}
    for s in range(nx):
        col = lax.rem(gx + s, nx) * cpl
        for g in range(ny):
            tile_loads[s, g] = pltpu.make_async_copy(
                tiles_hbm.at[pl.ds(g * rpd, rpd), pl.ds(col, cpl)],
                tiles.at[pl.ds(g * rpd, rpd), pl.ds(col, cpl)],
                tile_sem.at[s, g],
            )

    barrier = pltpu.get_barrier_semaphore()
    x_peers = [(lax.rem(gx + i, nx), gy, gz) for i in range(1, nx)]
    y_peers = [(gx, lax.rem(gy + j, ny), gz) for j in range(1, ny)]
    z_peers = [(gx, gy, lax.rem(gz + k, nz)) for k in range(1, nz)]
    xy_peers = [
        (lax.rem(gx + i, nx), lax.rem(gy + j, ny), gz)
        for i in range(nx) for j in range(ny) if i or j
    ]
    above, below = (gx, gy, gz + 1), (gx, gy, gz - 1)

    def signal(sem, peer):
        pl.semaphore_signal(sem, inc=1, device_id=peer, device_id_type=MESH)

    for peer in x_peers + y_peers:
        signal(barrier, peer)
    pl.when(gz < nz - 1)(lambda: signal(barrier, above))
    pl.when(gz > 0)(lambda: signal(barrier, below))
    loads[0].start()
    for g in range(ny):
        tile_loads[0, g].start()
    for load in loads[1:]:
        load.start()
    for s in range(1, nx):
        for g in range(ny):
            tile_loads[s, g].start()
    loads[0].wait()
    z_near = (gz < nz - 1).astype(jnp.int32) + (gz > 0).astype(jnp.int32)
    pl.semaphore_wait(barrier, len(x_peers) + len(y_peers) + z_near)

    x_copies = []
    for s in range(1, nx):
        copy = pltpu.make_async_remote_copy(
            src_ref=panel.at[gx], dst_ref=panel.at[gx],
            send_sem=x_send.at[s - 1], recv_sem=x_recv.at[s - 1],
            device_id=(lax.rem(gx + s, nx), gy, gz), device_id_type=MESH,
        )
        copy.start()
        x_copies.append(copy)

    pl.when((gz == 1) & (gz < nz - 1))(lambda: signal(up_sem, above))
    pl.when((gz == nz - 2) & (gz > 0))(lambda: signal(down_sem, below))

    loads[1].wait()
    w_rows[...] = weight[...].T
    for load in loads[2:]:
        load.wait()

    def product(r, src):
        lhs, rhs = [], []
        for j in range(cpl):
            flag = mask_ref[src * cpl + j, r].astype(f32)
            block = panel[src, :, j * tile_len:(j + 1) * tile_len]
            lhs.append(block * jnp.full(block.shape, flag, f32).astype(bf16))
            rhs.append(tiles[r, src * cpl + j])
        return lax.dot_general(
            jnp.concatenate(lhs, axis=1), jnp.concatenate(rhs, axis=1),
            (((1,), (1,)), ((), ())), preferred_element_type=f32,
        )

    for g in range(ny):
        tile_loads[0, g].wait()
        for i in range(rpd):
            acc[g * rpd + i] = product(g * rpd + i, gx)

    @pl.when(gz > 1)
    def _():
        pl.semaphore_wait(up_sem, 1)
        pl.when(gz < nz - 1)(lambda: signal(up_sem, above))

    @pl.when(gz < nz - 2)
    def _():
        pl.semaphore_wait(down_sem, 1)
        pl.when(gz > 0)(lambda: signal(down_sem, below))

    for s in range(1, nx):
        for g in range(ny):
            tile_loads[s, g].wait()
        src = lax.rem(gx + nx - s, nx)
        x_copies[s - 1].wait()
        if s < nx - 1:
            for r in range(rows_blk):
                acc[r] += product(r, src)
    last = lax.rem(gx + 1, nx)

    y_copies = {}
    for h in range(chunks):
        for k in list(range(1, ny)) + [0]:
            dest = lax.rem(gy + k, ny)
            for i in range(rc):
                r = dest * rpd + h * rc + i
                total = acc[r]
                if nx > 1:
                    total = total + product(r, last)
                count = jnp.full((1, tile_len), count_ref[r].astype(f32), f32)
                total = total * (1.0 / count)
                cols = slice(i * tile_len, (i + 1) * tile_len)
                if k:
                    part_out[k - 1, h, :, cols] = total.astype(bf16)
                else:
                    mine[h, :, cols] = total
            if k:
                copy = pltpu.make_async_remote_copy(
                    src_ref=part_out.at[k - 1, h], dst_ref=part_in.at[k - 1, h],
                    send_sem=y_send.at[k - 1, h], recv_sem=y_recv.at[k - 1, h],
                    device_id=(gx, dest, gz), device_id_type=MESH,
                )
                copy.start()
                y_copies[k, h] = copy

    z_copies = {}
    ch = pl.ds(pl.multiple_of(gz * local_ch, local_ch), local_ch)
    for h in range(chunks):
        total = mine[h]
        for k in range(1, ny):
            y_copies[k, h].wait_recv()
            total = total + part_in[k - 1, h].astype(f32)
        full[h, ch, :] = total.astype(bf16)
        for k in range(1, nz):
            copy = pltpu.make_async_remote_copy(
                src_ref=full.at[h, ch], dst_ref=full.at[h, ch],
                send_sem=z_send.at[k - 1, h], recv_sem=z_recv.at[k - 1, h],
                device_id=z_peers[k - 1], device_id_type=MESH,
            )
            copy.start()
            z_copies[k, h] = copy

    w_local = w_rows[ch, :]
    sums = jnp.zeros((local_ch, 1), f32)
    squares = jnp.zeros((local_ch, 1), f32)
    for h in range(chunks):
        for k in range(1, nz):
            z_copies[k, h].wait_recv()
        z_vals = jnp.dot(w_local, full[h], preferred_element_type=f32)
        z_scr[h] = z_vals
        sums += jnp.sum(z_vals, axis=1, keepdims=True)
        squares += jnp.sum(z_vals * z_vals, axis=1, keepdims=True)
    lane = lax.broadcasted_iota(jnp.int32, (local_ch, 128), 1)
    stacked = jnp.where(lane == 0, sums, jnp.where(lane == 1, squares, 0.0))
    stat_out[...] = stacked.T[0:8, :]
    s_copies = []
    for k, peer in enumerate(xy_peers):
        copy = pltpu.make_async_remote_copy(
            src_ref=stat_out, dst_ref=stat_in.at[k],
            send_sem=s_send.at[k], recv_sem=s_recv.at[k],
            device_id=peer, device_id_type=MESH,
        )
        copy.start()
        s_copies.append(copy)
    stats = stat_out[...]
    for k, copy in enumerate(s_copies):
        copy.wait_recv()
        stats = stats + stat_in[k]
    nodes = span * chunks * nx * ny
    mean = stats[0:1, :] / nodes
    var = stats[1:2, :] / nodes - mean * mean
    scale = gamma[...] * lax.rsqrt(var + 1e-05)
    row = lax.broadcasted_iota(jnp.int32, (8, local_ch), 0)
    table = jnp.where(row == 0, mean, jnp.where(row == 1, scale, beta[...]))
    cols = table.T
    mean_c, scale_c, beta_c = cols[:, 0:1], cols[:, 1:2], cols[:, 2:3]
    for h in range(chunks):
        value = (z_scr[h] - mean_c) * scale_c + beta_c
        out_ref[:, h * span:(h + 1) * span] = jnp.maximum(value, 0.0).astype(bf16)

    for copy in list(y_copies.values()) + list(z_copies.values()) + s_copies:
        copy.wait_send()


def body(sizes, features, tiles, block_mask, tile_counts, weight, gamma, beta):
    nx, ny, nz = sizes
    local_ch, nodes = features.shape
    rows_blk, cols_blk, tile_len, _ = tiles.shape
    width = rows_blk * tile_len // ny
    rpd = rows_blk // ny
    chunks = CHUNKS if rpd % CHUNKS == 0 else 1
    span = width // chunks
    f32, bf16 = jnp.float32, jnp.bfloat16
    peers = nx * ny - 1
    dma = pltpu.SemaphoreType.DMA
    hbm = pl.BlockSpec(memory_space=pl.ANY)
    return pl.pallas_call(
        functools.partial(kernel, sizes, chunks),
        out_shape=pltpu.VMEM((local_ch, width), bf16),
        in_specs=[hbm] * 7,
        out_specs=pl.BlockSpec(memory_space=pltpu.VMEM),
        scratch_shapes=[
            pltpu.SMEM((cols_blk, rows_blk), jnp.int32),
            pltpu.SMEM((rows_blk,), jnp.int32),
            pltpu.VMEM((nx, local_ch, nodes), bf16),
            pltpu.VMEM(tiles.shape, bf16),
            pltpu.VMEM(weight.shape, bf16),
            pltpu.VMEM(weight.shape[::-1], bf16),
            pltpu.VMEM((1, local_ch), f32),
            pltpu.VMEM((1, local_ch), f32),
            pltpu.VMEM((rows_blk, local_ch, tile_len), f32),
            pltpu.VMEM((chunks, local_ch, span), f32),
            pltpu.VMEM((max(ny - 1, 1), chunks, local_ch, span), bf16),
            pltpu.VMEM((max(ny - 1, 1), chunks, local_ch, span), bf16),
            pltpu.VMEM((chunks, local_ch * nz, span), bf16),
            pltpu.VMEM((chunks, local_ch, span), f32),
            pltpu.VMEM((8, local_ch), f32),
            pltpu.VMEM((max(peers, 1), 8, local_ch), f32),
            dma((6,)),
            dma((nx, ny)),
            pltpu.SemaphoreType.REGULAR,
            pltpu.SemaphoreType.REGULAR,
            dma((max(nx - 1, 1),)),
            dma((max(nx - 1, 1),)),
            dma((max(ny - 1, 1), chunks)),
            dma((max(ny - 1, 1), chunks)),
            dma((max(nz - 1, 1), chunks)),
            dma((max(nz - 1, 1), chunks)),
            dma((max(peers, 1),)),
            dma((max(peers, 1),)),
        ],
        compiler_params=pltpu.CompilerParams(collective_id=0, has_side_effects=True),
        name="graph_conv",
    )(features, tiles, block_mask.T, tile_counts, weight,
      gamma.reshape(1, local_ch), beta.reshape(1, local_ch))


def solution(mesh):
    in_specs = (
        P("gz", ("gy", "gx")),
        P("gx", "gy", None, None),
        P("gx", "gy"),
        P("gx"),
        P(),
        P("gz"),
        P("gz"),
    )
    out_specs = P("gz", ("gx", "gy"))
    sizes = tuple(mesh.shape[name] for name in ("gx", "gy", "gz"))
    return jax.shard_map(
        functools.partial(body, sizes), mesh=mesh, in_specs=in_specs,
        out_specs=out_specs, check_vma=False,
    )
```

```python
import functools

import jax
import jax.numpy as jnp
from jax import lax
from jax.experimental import pallas as pl
from jax.experimental.pallas import tpu as pltpu
from jax.sharding import PartitionSpec as P

MESH = pl.DeviceIdType.MESH
CHUNKS = 2


def kernel(
    sizes, chunks,
    feat_hbm, tiles_hbm, mask_hbm, count_hbm, weight_hbm, gamma_hbm, beta_hbm,
    out_ref,
    mask_ref, count_ref, panel, tiles, weight, w_rows, gamma, beta, acc, mine, part_out, part_in, full, z_scr,
    edge_out, edge_in, stat_out, stat_in, stat_sum,
    load_sem, tile_sem, up_sem, down_sem, x_send, x_recv, y_send, y_recv, z_send, z_recv, e_send, e_recv, s_send, s_recv,
):
    nx, ny, nz = sizes
    gx, gy, gz = lax.axis_index("gx"), lax.axis_index("gy"), lax.axis_index("gz")
    rows_blk, cols_blk, tile_len, _ = tiles.shape
    local_ch = panel.shape[1]
    cpl = cols_blk // nx
    rpd = rows_blk // ny
    rc = rpd // chunks
    span = rc * tile_len
    f32, bf16 = jnp.float32, jnp.bfloat16

    loads = [
        pltpu.make_async_copy(feat_hbm, panel.at[gx], load_sem.at[0]),
        pltpu.make_async_copy(weight_hbm, weight, load_sem.at[1]),
        pltpu.make_async_copy(gamma_hbm, gamma, load_sem.at[2]),
        pltpu.make_async_copy(beta_hbm, beta, load_sem.at[3]),
        pltpu.make_async_copy(mask_hbm, mask_ref, load_sem.at[4]),
        pltpu.make_async_copy(count_hbm, count_ref, load_sem.at[5]),
    ]
    tile_loads = {}
    for s in range(nx):
        col = lax.rem(gx + s, nx) * cpl
        for g in range(ny):
            tile_loads[s, g] = pltpu.make_async_copy(
                tiles_hbm.at[pl.ds(g * rpd, rpd), pl.ds(col, cpl)],
                tiles.at[pl.ds(g * rpd, rpd), pl.ds(col, cpl)],
                tile_sem.at[s, g],
            )

    barrier = pltpu.get_barrier_semaphore()
    x_peers = [(lax.rem(gx + i, nx), gy, gz) for i in range(1, nx)]
    y_peers = [(gx, lax.rem(gy + j, ny), gz) for j in range(1, ny)]
    xy_peers = [
        (lax.rem(gx + i, nx), lax.rem(gy + j, ny), gz)
        for i in range(nx) for j in range(ny) if i or j
    ]
    above, below = (gx, gy, gz + 1), (gx, gy, gz - 1)

    def signal(sem, peer):
        pl.semaphore_signal(sem, inc=1, device_id=peer, device_id_type=MESH)

    for peer in x_peers + y_peers:
        signal(barrier, peer)
    pl.when(gz < nz - 1)(lambda: signal(barrier, above))
    pl.when(gz > 0)(lambda: signal(barrier, below))
    loads[0].start()
    for g in range(ny):
        tile_loads[0, g].start()
    for load in loads[1:]:
        load.start()
    for s in range(1, nx):
        for g in range(ny):
            tile_loads[s, g].start()
    loads[0].wait()
    z_near = (gz < nz - 1).astype(jnp.int32) + (gz > 0).astype(jnp.int32)
    pl.semaphore_wait(barrier, len(x_peers) + len(y_peers) + z_near)

    x_copies = []
    for s in range(1, nx):
        copy = pltpu.make_async_remote_copy(
            src_ref=panel.at[gx], dst_ref=panel.at[gx],
            send_sem=x_send.at[s - 1], recv_sem=x_recv.at[s - 1],
            device_id=(lax.rem(gx + s, nx), gy, gz), device_id_type=MESH,
        )
        copy.start()
        x_copies.append(copy)

    pl.when((gz == 1) & (gz < nz - 1))(lambda: signal(up_sem, above))
    pl.when((gz == nz - 2) & (gz > 0))(lambda: signal(down_sem, below))

    loads[1].wait()
    w_rows[...] = weight[...].T
    for load in loads[2:]:
        load.wait()

    def product(r, src):
        lhs, rhs = [], []
        for j in range(cpl):
            flag = mask_ref[src * cpl + j, r].astype(f32)
            block = panel[src, :, j * tile_len:(j + 1) * tile_len]
            lhs.append(block * jnp.full(block.shape, flag, f32).astype(bf16))
            rhs.append(tiles[r, src * cpl + j])
        return lax.dot_general(
            jnp.concatenate(lhs, axis=1), jnp.concatenate(rhs, axis=1),
            (((1,), (1,)), ((), ())), preferred_element_type=f32,
        )

    for g in range(ny):
        tile_loads[0, g].wait()
        for i in range(rpd):
            acc[g * rpd + i] = product(g * rpd + i, gx)

    @pl.when(gz > 1)
    def _():
        pl.semaphore_wait(up_sem, 1)
        pl.when(gz < nz - 1)(lambda: signal(up_sem, above))

    @pl.when(gz < nz - 2)
    def _():
        pl.semaphore_wait(down_sem, 1)
        pl.when(gz > 0)(lambda: signal(down_sem, below))

    for s in range(1, nx):
        for g in range(ny):
            tile_loads[s, g].wait()
        src = lax.rem(gx + nx - s, nx)
        x_copies[s - 1].wait()
        if s < nx - 1:
            for r in range(rows_blk):
                acc[r] += product(r, src)
    last = lax.rem(gx + 1, nx)

    y_copies = {}
    for h in range(chunks):
        for k in list(range(1, ny)) + [0]:
            dest = lax.rem(gy + k, ny)
            for i in range(rc):
                r = dest * rpd + h * rc + i
                total = acc[r]
                if nx > 1:
                    total = total + product(r, last)
                count = jnp.full((1, tile_len), count_ref[r].astype(f32), f32)
                total = total * (1.0 / count)
                cols = slice(i * tile_len, (i + 1) * tile_len)
                if k:
                    part_out[k - 1, h, :, cols] = total.astype(bf16)
                else:
                    mine[h, :, cols] = total
            if k:
                copy = pltpu.make_async_remote_copy(
                    src_ref=part_out.at[k - 1, h], dst_ref=part_in.at[k - 1, h],
                    send_sem=y_send.at[k - 1, h], recv_sem=y_recv.at[k - 1, h],
                    device_id=(gx, dest, gz), device_id_type=MESH,
                )
                copy.start()
                y_copies[k, h] = copy

    ch = pl.ds(pl.multiple_of(gz * local_ch, local_ch), local_ch)
    hubs = nz == 4
    first = jnp.where(gz < 2, 2, 1)
    edge = jnp.where(gz == 1, 0, nz - 1)
    is_hub = (gz == 1) | (gz == 2)

    def row_copy(h, slot, source, dest):
        rows = pl.ds(pl.multiple_of(source * local_ch, local_ch), local_ch)
        return pltpu.make_async_remote_copy(
            src_ref=full.at[h, rows], dst_ref=full.at[h, rows],
            send_sem=z_send.at[slot, h], recv_sem=z_recv.at[source, h],
            device_id=(gx, gy, dest), device_id_type=MESH,
        )

    def gather_copies(h):
        if hubs:
            return [row_copy(h, 0, gz, first)], row_copy(h, 1, gz, 3 - first)
        return [row_copy(h, k - 1, gz, lax.rem(gz + k, nz)) for k in range(1, nz)], None

    for h in range(chunks):
        total = mine[h]
        for k in range(1, ny):
            y_copies[k, h].wait_recv()
            total = total + part_in[k - 1, h].astype(f32)
        full[h, ch, :] = total.astype(bf16)
        always, outer = gather_copies(h)
        for copy in always:
            copy.start()
        if hubs:
            pl.when(jnp.logical_not(is_hub))(outer.start)

    def wait_rows(h):
        for k in range(1, nz):
            row_copy(h, 0, lax.rem(gz + k, nz), gz).wait_recv()

    def channel_sums(vals):
        return jnp.sum(vals, axis=1, keepdims=True), jnp.sum(vals * vals, axis=1, keepdims=True)

    lane = lax.broadcasted_iota(jnp.int32, (local_ch, 128), 1)

    def as_rows(columns):
        stacked = jnp.zeros((local_ch, 128), f32)
        for n, column in enumerate(columns):
            stacked = jnp.where(lane == n, column, stacked)
        return stacked.T[0:8, :]

    npeer = len(xy_peers)

    def stat_copy(which, k, peer):
        return pltpu.make_async_remote_copy(
            src_ref=stat_out.at[which], dst_ref=stat_in.at[k],
            send_sem=s_send.at[which, k], recv_sem=s_recv.at[k],
            device_id=peer, device_id_type=MESH,
        )

    def edge_copy(h, dest):
        return pltpu.make_async_remote_copy(
            src_ref=edge_out.at[h], dst_ref=edge_in.at[h],
            send_sem=e_send.at[h], recv_sem=e_recv.at[h],
            device_id=(gx, gy, dest), device_id_type=MESH,
        )

    own_stats = [stat_copy(0, k, peer) for k, peer in enumerate(xy_peers)]
    edge_stats = [stat_copy(1, k, (peer[0], peer[1], edge)) for k, peer in enumerate(xy_peers)]
    edge_stats.append(stat_copy(1, npeer, (gx, gy, edge)))

    def whole_rows():
        edge_ch = pl.ds(pl.multiple_of(edge * local_ch, local_ch), local_ch)
        sums, squares, far_sums, far_squares, means = 0.0, 0.0, 0.0, 0.0, []
        for h in range(chunks):
            wait_rows(h)
            if hubs:
                z_far = jnp.dot(w_rows[edge_ch, :], full[h], preferred_element_type=f32)
                s, q = channel_sums(z_far)
                far_sums, far_squares = far_sums + s, far_squares + q
                means.append(s / span)
                edge_out[h] = (z_far - means[h]).astype(bf16)
                edge_copy(h, edge).start()
            if hubs and h == chunks - 1:
                stat_out[1] = as_rows([far_sums, far_squares] + means)
                for copy in edge_stats:
                    copy.start()
            z_vals = jnp.dot(w_rows[ch, :], full[h], preferred_element_type=f32)
            z_scr[h] = z_vals
            s, q = channel_sums(z_vals)
            sums, squares = sums + s, squares + q
        stat_out[0] = as_rows([sums, squares])
        for copy in own_stats:
            copy.start()
        stats = stat_out[0]
        for k, copy in enumerate(own_stats):
            copy.wait_recv()
            stats = stats + stat_in[k]
        stat_sum[...] = stats

    def edge_rows():
        mine_rows = lax.broadcasted_iota(jnp.int32, (8, local_ch), 0) < 2
        edge_stats[npeer].wait_recv()
        stats = stat_in[npeer]
        for k in range(npeer):
            edge_stats[k].wait_recv()
            stats = stats + jnp.where(mine_rows, stat_in[k], 0.0)
        stat_sum[...] = stats
        for h in range(chunks):
            edge_copy(h, edge).wait_recv()
            z_scr[h] = edge_in[h].astype(f32)

    if hubs:
        pl.when(is_hub)(whole_rows)
        pl.when(jnp.logical_not(is_hub))(edge_rows)
    else:
        whole_rows()

    nodes = span * chunks * nx * ny
    stats = stat_sum[...]
    mean = stats[0:1, :] / nodes
    var = stats[1:2, :] / nodes - mean * mean
    scale = gamma[...] * lax.rsqrt(var + 1e-05)
    row = lax.broadcasted_iota(jnp.int32, (8, local_ch), 0)
    table = jnp.where(row == 0, scale, jnp.where(row == 1, beta[...], stats - mean))
    cols = table.T
    for h in range(chunks):
        value = (z_scr[h] + cols[:, 2 + h:3 + h]) * cols[:, 0:1] + cols[:, 1:2]
        out_ref[:, h * span:(h + 1) * span] = jnp.maximum(value, 0.0).astype(bf16)

    for copy in y_copies.values():
        copy.wait_send()
    for h in range(chunks):
        always, outer = gather_copies(h)
        for copy in always:
            copy.wait_send()
        if hubs:
            pl.when(jnp.logical_not(is_hub))(outer.wait_send)

    def finish():
        for copy in own_stats:
            copy.wait_send()
        if hubs:
            for copy in edge_stats:
                copy.wait_send()
            for h in range(chunks):
                edge_copy(h, edge).wait_send()

    if hubs:
        pl.when(is_hub)(finish)
    else:
        finish()


def body(sizes, features, tiles, block_mask, tile_counts, weight, gamma, beta):
    nx, ny, nz = sizes
    local_ch, nodes = features.shape
    rows_blk, cols_blk, tile_len, _ = tiles.shape
    width = rows_blk * tile_len // ny
    rpd = rows_blk // ny
    chunks = CHUNKS if rpd % CHUNKS == 0 else 1
    span = width // chunks
    f32, bf16 = jnp.float32, jnp.bfloat16
    peers = nx * ny - 1
    dma = pltpu.SemaphoreType.DMA
    hbm = pl.BlockSpec(memory_space=pl.ANY)
    return pl.pallas_call(
        functools.partial(kernel, sizes, chunks),
        out_shape=pltpu.VMEM((local_ch, width), bf16),
        in_specs=[hbm] * 7,
        out_specs=pl.BlockSpec(memory_space=pltpu.VMEM),
        scratch_shapes=[
            pltpu.SMEM((cols_blk, rows_blk), jnp.int32),
            pltpu.SMEM((rows_blk,), jnp.int32),
            pltpu.VMEM((nx, local_ch, nodes), bf16),
            pltpu.VMEM(tiles.shape, bf16),
            pltpu.VMEM(weight.shape, bf16),
            pltpu.VMEM(weight.shape[::-1], bf16),
            pltpu.VMEM((1, local_ch), f32),
            pltpu.VMEM((1, local_ch), f32),
            pltpu.VMEM((rows_blk, local_ch, tile_len), f32),
            pltpu.VMEM((chunks, local_ch, span), f32),
            pltpu.VMEM((max(ny - 1, 1), chunks, local_ch, span), bf16),
            pltpu.VMEM((max(ny - 1, 1), chunks, local_ch, span), bf16),
            pltpu.VMEM((chunks, local_ch * nz, span), bf16),
            pltpu.VMEM((chunks, local_ch, span), f32),
            pltpu.VMEM((chunks, local_ch, span), bf16),
            pltpu.VMEM((chunks, local_ch, span), bf16),
            pltpu.VMEM((2, 8, local_ch), f32),
            pltpu.VMEM((peers + 1, 8, local_ch), f32),
            pltpu.VMEM((8, local_ch), f32),
            dma((6,)),
            dma((nx, ny)),
            pltpu.SemaphoreType.REGULAR,
            pltpu.SemaphoreType.REGULAR,
            dma((max(nx - 1, 1),)),
            dma((max(nx - 1, 1),)),
            dma((max(ny - 1, 1), chunks)),
            dma((max(ny - 1, 1), chunks)),
            dma((max(nz - 1, 2), chunks)),
            dma((nz, chunks)),
            dma((chunks,)),
            dma((chunks,)),
            dma((2, peers + 1)),
            dma((peers + 1,)),
        ],
        compiler_params=pltpu.CompilerParams(collective_id=0, has_side_effects=True),
        name="graph_conv",
    )(features, tiles, block_mask.T, tile_counts, weight,
      gamma.reshape(1, local_ch), beta.reshape(1, local_ch))


def solution(mesh):
    in_specs = (
        P("gz", ("gy", "gx")),
        P("gx", "gy", None, None),
        P("gx", "gy"),
        P("gx"),
        P(),
        P("gz"),
        P("gz"),
    )
    out_specs = P("gz", ("gx", "gy"))
    sizes = tuple(mesh.shape[name] for name in ("gx", "gy", "gz"))
    return jax.shard_map(
        functools.partial(body, sizes), mesh=mesh, in_specs=in_specs,
        out_specs=out_specs, check_vma=False,
    )
```

```python
import functools

import jax
import jax.numpy as jnp
from jax import lax
from jax.experimental import pallas as pl
from jax.experimental.pallas import tpu as pltpu
from jax.sharding import PartitionSpec as P

MESH = pl.DeviceIdType.MESH
CHUNKS = 2


def kernel(
    sizes, chunks,
    feat_hbm, tiles_hbm, mask_hbm, count_hbm, weight_hbm, gamma_hbm, beta_hbm,
    out_ref,
    mask_ref, count_ref, panel, tiles, weight, w_rows, gamma, beta, acc, mine, part_out, part_in, full, z_scr,
    edge_out, edge_in, stat_out, stat_in, stat_sum,
    load_sem, tile_sem, up_sem, down_sem, x_send, x_recv, y_send, y_recv, z_send, z_recv, e_send, e_recv, s_send, s_recv,
):
    nx, ny, nz = sizes
    gx, gy, gz = lax.axis_index("gx"), lax.axis_index("gy"), lax.axis_index("gz")
    rows_blk, cols_blk, tile_len, _ = tiles.shape
    local_ch = panel.shape[1]
    cpl = cols_blk // nx
    rpd = rows_blk // ny
    rc = rpd // chunks
    span = rc * tile_len
    f32, bf16 = jnp.float32, jnp.bfloat16

    loads = [
        pltpu.make_async_copy(feat_hbm, panel.at[gx], load_sem.at[0]),
        pltpu.make_async_copy(weight_hbm, weight, load_sem.at[1]),
        pltpu.make_async_copy(gamma_hbm, gamma, load_sem.at[2]),
        pltpu.make_async_copy(beta_hbm, beta, load_sem.at[3]),
        pltpu.make_async_copy(mask_hbm, mask_ref, load_sem.at[4]),
        pltpu.make_async_copy(count_hbm, count_ref, load_sem.at[5]),
    ]
    tile_loads = {}
    for s in range(nx):
        col = lax.rem(gx + s, nx) * cpl
        for g in range(ny):
            tile_loads[s, g] = pltpu.make_async_copy(
                tiles_hbm.at[pl.ds(g * rpd, rpd), pl.ds(col, cpl)],
                tiles.at[pl.ds(g * rpd, rpd), pl.ds(col, cpl)],
                tile_sem.at[s, g],
            )

    barrier = pltpu.get_barrier_semaphore()
    x_peers = [(lax.rem(gx + i, nx), gy, gz) for i in range(1, nx)]
    y_peers = [(gx, lax.rem(gy + j, ny), gz) for j in range(1, ny)]
    xy_peers = [
        (lax.rem(gx + i, nx), lax.rem(gy + j, ny), gz)
        for i in range(nx) for j in range(ny) if i or j
    ]
    above, below = (gx, gy, gz + 1), (gx, gy, gz - 1)

    def signal(sem, peer):
        pl.semaphore_signal(sem, inc=1, device_id=peer, device_id_type=MESH)

    for peer in x_peers + y_peers:
        signal(barrier, peer)
    pl.when(gz < nz - 1)(lambda: signal(barrier, above))
    pl.when(gz > 0)(lambda: signal(barrier, below))
    loads[0].start()
    for g in range(ny):
        tile_loads[0, g].start()
    for load in loads[1:]:
        load.start()
    for s in range(1, nx):
        for g in range(ny):
            tile_loads[s, g].start()
    loads[0].wait()
    z_near = (gz < nz - 1).astype(jnp.int32) + (gz > 0).astype(jnp.int32)
    pl.semaphore_wait(barrier, len(x_peers) + len(y_peers) + z_near)

    x_copies = []
    for s in range(1, nx):
        copy = pltpu.make_async_remote_copy(
            src_ref=panel.at[gx], dst_ref=panel.at[gx],
            send_sem=x_send.at[s - 1], recv_sem=x_recv.at[s - 1],
            device_id=(lax.rem(gx + s, nx), gy, gz), device_id_type=MESH,
        )
        copy.start()
        x_copies.append(copy)

    pl.when((gz == 1) & (gz < nz - 1))(lambda: signal(up_sem, above))
    pl.when((gz == nz - 2) & (gz > 0))(lambda: signal(down_sem, below))

    loads[1].wait()
    w_rows[...] = weight[...].T
    for load in loads[2:]:
        load.wait()

    def product(r, src):
        lhs, rhs = [], []
        for j in range(cpl):
            flag = mask_ref[src * cpl + j, r].astype(f32)
            block = panel[src, :, j * tile_len:(j + 1) * tile_len]
            lhs.append(block * jnp.full(block.shape, flag, f32).astype(bf16))
            rhs.append(tiles[r, src * cpl + j])
        return lax.dot_general(
            jnp.concatenate(lhs, axis=1), jnp.concatenate(rhs, axis=1),
            (((1,), (1,)), ((), ())), preferred_element_type=f32,
        )

    for g in range(ny):
        tile_loads[0, g].wait()
        for i in range(rpd):
            acc[g * rpd + i] = product(g * rpd + i, gx)

    @pl.when(gz > 1)
    def _():
        pl.semaphore_wait(up_sem, 1)
        pl.when(gz < nz - 1)(lambda: signal(up_sem, above))

    @pl.when(gz < nz - 2)
    def _():
        pl.semaphore_wait(down_sem, 1)
        pl.when(gz > 0)(lambda: signal(down_sem, below))

    for s in range(1, nx):
        for g in range(ny):
            tile_loads[s, g].wait()
        src = lax.rem(gx + nx - s, nx)
        x_copies[s - 1].wait()
        if s < nx - 1:
            for r in range(rows_blk):
                acc[r] += product(r, src)
    last = lax.rem(gx + 1, nx)

    y_copies = {}
    for h in range(chunks):
        for k in list(range(1, ny)) + [0]:
            dest = lax.rem(gy + k, ny)
            for i in range(rc):
                r = dest * rpd + h * rc + i
                total = acc[r]
                if nx > 1:
                    total = total + product(r, last)
                count = jnp.full((1, tile_len), count_ref[r].astype(f32), f32)
                total = total * (1.0 / count)
                cols = slice(i * tile_len, (i + 1) * tile_len)
                if k:
                    part_out[k - 1, h, :, cols] = total.astype(bf16)
                else:
                    mine[h, :, cols] = total
            if k:
                copy = pltpu.make_async_remote_copy(
                    src_ref=part_out.at[k - 1, h], dst_ref=part_in.at[k - 1, h],
                    send_sem=y_send.at[k - 1, h], recv_sem=y_recv.at[k - 1, h],
                    device_id=(gx, dest, gz), device_id_type=MESH,
                )
                copy.start()
                y_copies[k, h] = copy

    ch = pl.ds(pl.multiple_of(gz * local_ch, local_ch), local_ch)
    hubs = nz == 4
    first = jnp.where(gz < 2, 2, 1)
    edge = jnp.where(gz == 1, 0, nz - 1)
    is_hub = (gz == 1) | (gz == 2)

    def row_copy(h, slot, source, dest):
        rows = pl.ds(pl.multiple_of(source * local_ch, local_ch), local_ch)
        return pltpu.make_async_remote_copy(
            src_ref=full.at[h, rows], dst_ref=full.at[h, rows],
            send_sem=z_send.at[slot, h], recv_sem=z_recv.at[source, h],
            device_id=(gx, gy, dest), device_id_type=MESH,
        )

    def gather_copies(h):
        if hubs:
            return [row_copy(h, 0, gz, first)], row_copy(h, 1, gz, 3 - first)
        return [row_copy(h, k - 1, gz, lax.rem(gz + k, nz)) for k in range(1, nz)], None

    for h in range(chunks):
        total = mine[h]
        for k in range(1, ny):
            y_copies[k, h].wait_recv()
            total = total + part_in[k - 1, h].astype(f32)
        full[h, ch, :] = total.astype(bf16)
        always, outer = gather_copies(h)
        for copy in always:
            copy.start()
        if hubs:
            pl.when(jnp.logical_not(is_hub))(outer.start)

    def wait_rows(h):
        for k in range(1, nz):
            row_copy(h, 0, lax.rem(gz + k, nz), gz).wait_recv()

    def channel_sums(vals):
        return jnp.sum(vals, axis=1, keepdims=True), jnp.sum(vals * vals, axis=1, keepdims=True)

    lane = lax.broadcasted_iota(jnp.int32, (local_ch, 128), 1)

    def as_rows(columns):
        stacked = jnp.zeros((local_ch, 128), f32)
        for n, column in enumerate(columns):
            stacked = jnp.where(lane == n, column, stacked)
        return stacked.T[0:8, :]

    npeer = len(xy_peers)

    def stat_copy(which, k, peer):
        return pltpu.make_async_remote_copy(
            src_ref=stat_out.at[which], dst_ref=stat_in.at[k],
            send_sem=s_send.at[which, k], recv_sem=s_recv.at[k],
            device_id=peer, device_id_type=MESH,
        )

    def edge_copy(h, dest):
        return pltpu.make_async_remote_copy(
            src_ref=edge_out.at[h], dst_ref=edge_in.at[h],
            send_sem=e_send.at[h], recv_sem=e_recv.at[h],
            device_id=(gx, gy, dest), device_id_type=MESH,
        )

    own_stats = [stat_copy(0, k, peer) for k, peer in enumerate(xy_peers)]
    edge_stats = [stat_copy(1, k, (peer[0], peer[1], edge)) for k, peer in enumerate(xy_peers)]
    edge_stats.append(stat_copy(1, npeer, (gx, gy, edge)))

    def whole_rows():
        edge_ch = pl.ds(pl.multiple_of(edge * local_ch, local_ch), local_ch)
        sums, squares, far_sums, far_squares, means = 0.0, 0.0, 0.0, 0.0, []
        for h in range(chunks):
            wait_rows(h)
            if hubs:
                z_far = jnp.dot(w_rows[edge_ch, :], full[h], preferred_element_type=f32)
                s, q = channel_sums(z_far)
                far_sums, far_squares = far_sums + s, far_squares + q
                means.append(s / span)
                edge_out[h] = (z_far - means[h]).astype(bf16)
            if hubs and h < chunks - 1:
                edge_copy(h, edge).start()
            if hubs and h == chunks - 1:
                stat_out[1] = as_rows([far_sums, far_squares] + means)
                for copy in edge_stats:
                    copy.start()
                edge_copy(h, edge).start()
            z_vals = jnp.dot(w_rows[ch, :], full[h], preferred_element_type=f32)
            z_scr[h] = z_vals
            s, q = channel_sums(z_vals)
            sums, squares = sums + s, squares + q
        stat_out[0] = as_rows([sums, squares])
        for copy in own_stats:
            copy.start()
        stats = stat_out[0]
        for k, copy in enumerate(own_stats):
            copy.wait_recv()
            stats = stats + stat_in[k]
        stat_sum[...] = stats

    def edge_rows():
        mine_rows = lax.broadcasted_iota(jnp.int32, (8, local_ch), 0) < 2
        edge_stats[npeer].wait_recv()
        stats = stat_in[npeer]
        for k in range(npeer):
            edge_stats[k].wait_recv()
            stats = stats + jnp.where(mine_rows, stat_in[k], 0.0)
        stat_sum[...] = stats
        for h in range(chunks):
            edge_copy(h, edge).wait_recv()
            z_scr[h] = edge_in[h].astype(f32)

    if hubs:
        pl.when(is_hub)(whole_rows)
        pl.when(jnp.logical_not(is_hub))(edge_rows)
    else:
        whole_rows()

    nodes = span * chunks * nx * ny
    stats = stat_sum[...]
    mean = stats[0:1, :] / nodes
    var = stats[1:2, :] / nodes - mean * mean
    scale = gamma[...] * lax.rsqrt(var + 1e-05)
    row = lax.broadcasted_iota(jnp.int32, (8, local_ch), 0)
    table = jnp.where(row == 0, scale, jnp.where(row == 1, beta[...], stats - mean))
    cols = table.T
    for h in range(chunks):
        value = (z_scr[h] + cols[:, 2 + h:3 + h]) * cols[:, 0:1] + cols[:, 1:2]
        out_ref[:, h * span:(h + 1) * span] = jnp.maximum(value, 0.0).astype(bf16)

    for copy in y_copies.values():
        copy.wait_send()
    for h in range(chunks):
        always, outer = gather_copies(h)
        for copy in always:
            copy.wait_send()
        if hubs:
            pl.when(jnp.logical_not(is_hub))(outer.wait_send)

    def finish():
        for copy in own_stats:
            copy.wait_send()
        if hubs:
            for copy in edge_stats:
                copy.wait_send()
            for h in range(chunks):
                edge_copy(h, edge).wait_send()

    if hubs:
        pl.when(is_hub)(finish)
    else:
        finish()


def body(sizes, features, tiles, block_mask, tile_counts, weight, gamma, beta):
    nx, ny, nz = sizes
    local_ch, nodes = features.shape
    rows_blk, cols_blk, tile_len, _ = tiles.shape
    width = rows_blk * tile_len // ny
    rpd = rows_blk // ny
    chunks = CHUNKS if rpd % CHUNKS == 0 else 1
    span = width // chunks
    f32, bf16 = jnp.float32, jnp.bfloat16
    peers = nx * ny - 1
    dma = pltpu.SemaphoreType.DMA
    hbm = pl.BlockSpec(memory_space=pl.ANY)
    return pl.pallas_call(
        functools.partial(kernel, sizes, chunks),
        out_shape=pltpu.VMEM((local_ch, width), bf16),
        in_specs=[hbm] * 7,
        out_specs=pl.BlockSpec(memory_space=pltpu.VMEM),
        scratch_shapes=[
            pltpu.SMEM((cols_blk, rows_blk), jnp.int32),
            pltpu.SMEM((rows_blk,), jnp.int32),
            pltpu.VMEM((nx, local_ch, nodes), bf16),
            pltpu.VMEM(tiles.shape, bf16),
            pltpu.VMEM(weight.shape, bf16),
            pltpu.VMEM(weight.shape[::-1], bf16),
            pltpu.VMEM((1, local_ch), f32),
            pltpu.VMEM((1, local_ch), f32),
            pltpu.VMEM((rows_blk, local_ch, tile_len), f32),
            pltpu.VMEM((chunks, local_ch, span), f32),
            pltpu.VMEM((max(ny - 1, 1), chunks, local_ch, span), bf16),
            pltpu.VMEM((max(ny - 1, 1), chunks, local_ch, span), bf16),
            pltpu.VMEM((chunks, local_ch * nz, span), bf16),
            pltpu.VMEM((chunks, local_ch, span), f32),
            pltpu.VMEM((chunks, local_ch, span), bf16),
            pltpu.VMEM((chunks, local_ch, span), bf16),
            pltpu.VMEM((2, 8, local_ch), f32),
            pltpu.VMEM((peers + 1, 8, local_ch), f32),
            pltpu.VMEM((8, local_ch), f32),
            dma((6,)),
            dma((nx, ny)),
            pltpu.SemaphoreType.REGULAR,
            pltpu.SemaphoreType.REGULAR,
            dma((max(nx - 1, 1),)),
            dma((max(nx - 1, 1),)),
            dma((max(ny - 1, 1), chunks)),
            dma((max(ny - 1, 1), chunks)),
            dma((max(nz - 1, 2), chunks)),
            dma((nz, chunks)),
            dma((chunks,)),
            dma((chunks,)),
            dma((2, peers + 1)),
            dma((peers + 1,)),
        ],
        compiler_params=pltpu.CompilerParams(collective_id=0, has_side_effects=True),
        name="graph_conv",
    )(features, tiles, block_mask.T, tile_counts, weight,
      gamma.reshape(1, local_ch), beta.reshape(1, local_ch))


def solution(mesh):
    in_specs = (
        P("gz", ("gy", "gx")),
        P("gx", "gy", None, None),
        P("gx", "gy"),
        P("gx"),
        P(),
        P("gz"),
        P("gz"),
    )
    out_specs = P("gz", ("gx", "gy"))
    sizes = tuple(mesh.shape[name] for name in ("gx", "gy", "gz"))
    return jax.shard_map(
        functools.partial(body, sizes), mesh=mesh, in_specs=in_specs,
        out_specs=out_specs, check_vma=False,
    )
```
